8 devices in a mesh: rep: 1 (over z), dp: 8 (over x, y, core).
Axes of the slice: x: 2, y: 2, z: 1, core: 2. Of those that a mesh axis runs over, the one named last changes fastest.
Arguments:
- x: bfloat16 [8, 2048, 1024], P(('rep', 'dp'))
- dy: bfloat16 [8, 2048, 1024], P(('rep', 'dp'))
- w_gate: bfloat16 [2, 1024, 2816], replicated
- w_up: bfloat16 [2, 1024, 2816], replicated
- w_down: bfloat16 [2, 2816, 1024], replicated
- m_w_gate: float32 [2, 1024, 2816], replicated
- m_w_up: float32 [2, 1024, 2816], replicated
- m_w_down: float32 [2, 2816, 1024], replicated
- v_w_gate: float32 [2, 1024, 2816], replicated
- v_w_up: float32 [2, 1024, 2816], replicated
- v_w_down: float32 [2, 2816, 1024], replicated
Outputs:
- output 1: bfloat16 [2, 1024, 2816], P('rep')
- output 2: bfloat16 [2, 1024, 2816], P('rep')
- output 3: bfloat16 [2, 2816, 1024], P('rep')
- output 4: float32 [2, 1024, 2816], P('rep')
- output 5: float32 [2, 1024, 2816], P('rep')
- output 6: float32 [2, 2816, 1024], P('rep')
- output 7: float32 [2, 1024, 2816], P('rep')
- output 8: float32 [2, 1024, 2816], P('rep')
- output 9: float32 [2, 2816, 1024], P('rep')
All inputs are finite; a program needn't handle non-finite values.
Results may differ from the reference program's by a relative error of at most 0.022.
Values are sent between devices in bfloat16 or wider.
A program may use at most 2.75 GiB of HBM per device.

```python
import jax
import jax.numpy as jnp
from jax import lax

SEQUENCES = 8
TOKENS = 2048
D = 1024
FF = 2816
LAYERS = 2
NAMES = ("w_gate", "w_up", "w_down")
SHAPES = {"w_gate": (LAYERS, D, FF), "w_up": (LAYERS, D, FF), "w_down": (LAYERS, FF, D)}


def bump(key, n, height):
    away = (jnp.arange(n, dtype=jnp.int32) - jax.random.randint(key, (), 0, n, jnp.int32)) % n
    return jnp.where(away < n // 8, height, 1.0)


def together(key, own, strength):
    shared = jax.random.normal(key, own.shape[1:], jnp.float32)
    return (own + strength * shared) * lax.rsqrt(1 + strength * strength)


def setup_inputs(seed: int = 0, part: int = 0) -> dict:
    kx, kdy, ka, kb, kz, kf, kh, kl, *keys = jax.random.split(jax.random.key(seed), 8 + 3 * len(NAMES))
    kx, kdy, ka, kb = (jax.random.fold_in(k, part) for k in (kx, kdy, ka, kb))
    kw, km, kv = (keys[i::3] for i in range(3))
    shape = (SEQUENCES, TOKENS, D)
    much_x, much_dy = jax.random.uniform(kz, (2,), jnp.float32, 0.0, 1.0)
    loud = 2.0 ** jax.random.uniform(jax.random.fold_in(kz, 1), (), jnp.float32, -1.0, 2.0)
    layers = 2.0 ** jax.random.uniform(kl, (LAYERS, 1, 1), jnp.float32, -1.0, 1.0)
    x = together(ka, jax.random.normal(kx, shape, jnp.float32), much_x) * bump(kf, D, 4.0)
    dy = together(kb, jax.random.normal(kdy, shape, jnp.float32), much_dy)
    drawn = {"x": x.astype(jnp.bfloat16), "dy": (loud * dy * (SEQUENCES * TOKENS) ** -0.5).astype(jnp.bfloat16)}
    for key, name in zip(kw, NAMES, strict=True):
        w = jax.random.normal(key, SHAPES[name], jnp.float32) * SHAPES[name][1] ** -0.5
        drawn[name] = (w * {"w_gate": 1.0, "w_up": bump(kh, FF, 4.0), "w_down": layers}[name]).astype(jnp.bfloat16)
    for key, name in zip(km, NAMES, strict=True):
        drawn[f"m_{name}"] = 0.1 * jax.random.normal(key, SHAPES[name], jnp.float32)
    for key, name in zip(kv, NAMES, strict=True):
        drawn[f"v_{name}"] = jax.random.uniform(key, SHAPES[name], jnp.float32, 0.005, 0.015)
    return drawn


def matmul(a, w):
    return jnp.dot(a, w, preferred_element_type=jnp.float32).astype(jnp.bfloat16)


def normed(h):
    wide = h.astype(jnp.float32)
    scale = lax.rsqrt(jnp.mean(wide**2, -1, keepdims=True) + 1e-6)
    return (wide * scale).astype(jnp.bfloat16)


def layer(h, w):
    a = normed(h)
    gate = jnp.dot(a, w["w_gate"], preferred_element_type=jnp.float32)
    up = jnp.dot(a, w["w_up"], preferred_element_type=jnp.float32)
    return h + matmul((jax.nn.silu(gate) * up).astype(jnp.bfloat16), w["w_down"])


def adamw(w, m, v, g):
    m = 0.9 * m + 0.1 * g
    v = 0.95 * v + 0.05 * g * g
    step = m * lax.rsqrt(v + 1e-8) + 0.1 * w
    return (w - 0.02 * step).astype(jnp.bfloat16), m, v


def clipped(gradients, sum_of_squares, count):
    factor = jnp.minimum(1.0, 0.5 * lax.rsqrt(sum_of_squares / count + 1e-30))
    return [g * factor for g in gradients]


def stack(weights, h):
    return lax.scan(lambda h, w: (layer(h, w), None), h, weights)[0]


def reference(x, dy, w_gate, w_up, w_down, m_w_gate, m_w_up, m_w_down, v_w_gate, v_w_up, v_w_down):
    weights = dict(zip(NAMES, (w_gate, w_up, w_down), strict=True))

    def take(so_far, sequence):
        h, by_y = sequence
        _, back = jax.vjp(lambda w: stack(w, h), weights)
        return jax.tree.map(lambda total, term: total + term.astype(jnp.float32), so_far, back(by_y)[0]), None

    none_yet = {name: jnp.zeros(w.shape, jnp.float32) for name, w in weights.items()}
    by_weights, _ = lax.scan(take, none_yet, (x, dy))
    gradients = [by_weights[name].astype(jnp.bfloat16).astype(jnp.float32) for name in NAMES]
    gradients = clipped(gradients, sum(jnp.sum(g * g) for g in gradients), sum(g.size for g in gradients))
    new = [
        adamw(w.astype(jnp.float32), m, v, g)
        for w, m, v, g in zip((w_gate, w_up, w_down), (m_w_gate, m_w_up, m_w_down), (v_w_gate, v_w_up, v_w_down), gradients, strict=True)
    ]
    return tuple(one[which] for which in range(3) for one in new)
```

```python
import functools

import jax
import jax.numpy as jnp
from jax import lax
from jax.experimental import pallas as pl
from jax.experimental.pallas import tpu as pltpu
from jax.sharding import PartitionSpec as P

T, D, F, TILE = 2048, 1024, 2816, 256
NT = F // TILE
BLOCK = 512
NB = T // BLOCK
DRAIN = 4
BF, F32 = jnp.bfloat16, jnp.float32
MESH = pl.DeviceIdType.MESH
VMEM_LIMIT = 62 * 1024 * 1024


def dot(a, b):
    return jnp.dot(a, b, preferred_element_type=F32)


def dot_t(a, b):
    return lax.dot_general(a, b, (((1,), (1,)), ((), ())), preferred_element_type=F32)


def whole(shape):
    zeros = (0,) * len(shape)
    return pl.BlockSpec(shape, lambda *_: zeros, pipeline_mode=pl.Buffered(1))


def scale_of(wide):
    return lax.rsqrt(jnp.mean(wide * wide, -1, keepdims=True) + 1e-6)


def forward_kernel(x_ref, dy_ref, wg_ref, wu_ref, wd_ref, gate_ref, up_ref, h_ref, a_ref, a0t_ref, at_ref, dyt_ref, a0, act):
    s = pl.program_id(0)

    @pl.when(s == 0)
    def _():
        for b in range(NB):
            rows = slice(b * BLOCK, (b + 1) * BLOCK)
            wide = x_ref[rows, :].astype(F32)
            a0[rows, :] = (wide * scale_of(wide)).astype(BF)

    @pl.when(s < NT)
    def _():
        columns = pl.ds(pl.multiple_of(s * TILE, TILE), TILE)
        wg, wu = wg_ref[0], wu_ref[0]
        for b in range(NB):
            rows = slice(b * BLOCK, (b + 1) * BLOCK)
            gate = dot(a0[rows, :], wg)
            up = dot(a0[rows, :], wu)
            gate_ref[rows, :] = gate
            up_ref[rows, :] = up
            act[rows, columns] = (gate * lax.logistic(gate) * up).astype(BF)

    @pl.when(s >= NT)
    def _():
        rows = pl.ds(pl.multiple_of((s - NT) * BLOCK, BLOCK), BLOCK)
        out = dot(act[rows, :], wd_ref[0]).astype(BF)
        h = (x_ref[rows, :].astype(F32) + out.astype(F32)).astype(BF)
        h_ref[...] = h
        wide = h.astype(F32)
        a = (wide * scale_of(wide)).astype(BF)
        a_ref[...] = a
        at_ref[...] = a.T
        a0t_ref[...] = a0[rows, :].T
        dyt_ref[...] = dy_ref[...].T


def forward(x, dy, wg, wu, wd):
    tile = lambda s: jnp.minimum(s, NT - 1)
    block = lambda s: jnp.maximum(s - NT, 0)
    wspec = pl.BlockSpec((1, D, TILE), lambda s: (0, 0, tile(s)))
    fspec = pl.BlockSpec((T, TILE), lambda s: (0, tile(s)))
    rspec = pl.BlockSpec((BLOCK, D), lambda s: (block(s), 0))
    tspec = pl.BlockSpec((D, BLOCK), lambda s: (0, block(s)))
    flat = lambda shape, dtype: jax.ShapeDtypeStruct(shape, dtype)
    return pl.pallas_call(
        forward_kernel,
        grid=(NT + NB,),
        in_specs=[whole((T, D)), rspec, wspec, wspec, whole((1, F, D))],
        out_specs=[fspec, fspec, rspec, rspec, tspec, tspec, tspec],
        out_shape=[
            flat((T, F), F32), flat((T, F), F32), flat((T, D), BF), flat((T, D), BF),
            flat((D, T), BF), flat((D, T), BF), flat((D, T), BF),
        ],
        scratch_shapes=[pltpu.VMEM((T, D), BF), pltpu.VMEM((T, F), BF)],
        compiler_params=pltpu.CompilerParams(dimension_semantics=("arbitrary",), vmem_limit_bytes=VMEM_LIMIT),
        cost_estimate=pl.CostEstimate(flops=6 * T * D * F, bytes_accessed=100 << 20, transcendentals=T * F),
        name="forward",
    )(x, dy, wg, wu, wd)


COMM_SCRATCH = [
    pltpu.VMEM((2, 4, 3, 128, 128), BF),
    pltpu.VMEM((2, 4, 3, 128, 128), F32),
    pltpu.VMEM((2, 2, 4, 3, 128, 128), BF),
    pltpu.VMEM((2, 2, 2, 3, 128, 128), BF),
    pltpu.VMEM((2, 2, 2, 3, 128, 128), F32),
    pltpu.VMEM((4, 2, 2, 3, 128, 128), BF),
    pltpu.VMEM((2, 2, 3, 128, 128), BF),
    pltpu.VMEM((2, 2, 3, 128, 128), F32),
    pltpu.VMEM((4, 2, 3, 128, 128), BF),
    pltpu.SemaphoreType.DMA((2,)),
    pltpu.SemaphoreType.DMA((2,)),
    pltpu.SemaphoreType.DMA((2, 2)),
    pltpu.SemaphoreType.DMA((4, 2)),
    pltpu.SemaphoreType.DMA((2, 2)),
    pltpu.SemaphoreType.DMA((4, 2)),
]


class Scatter:
    def __init__(self, refs, fin_ref, ssq_ref):
        (self.send_c, self.keep_c, self.recv_c, self.send_1, self.keep_1, self.recv_1, self.send_2, self.keep_2, self.recv_2,
         self.cs, self.cr, self.s1, self.r1, self.s2, self.r2) = refs
        self.fin_ref, self.ssq_ref = fin_ref, ssq_ref
        me = lax.axis_index("dp")
        self.core, self.y, self.x = lax.rem(me, 2), lax.rem(me // 2, 2), me // 4
        self.by_core, self.by_y, self.by_x = me + 1 - 2 * self.core, me + 2 - 4 * self.y, me + 4 - 8 * self.x

    def enter(self):
        barrier = pltpu.get_barrier_semaphore()
        for other in (self.by_core, self.by_y, self.by_x):
            pl.semaphore_signal(barrier, inc=1, device_id={"dp": other}, device_id_type=MESH)
        pl.semaphore_wait(barrier, 3)
        self.ssq_ref[...] = jnp.zeros_like(self.ssq_ref)

    def copy_c(self, t):
        slot = lax.rem(t, 2)
        return pltpu.make_async_remote_copy(
            self.send_c, self.recv_c.at[slot], self.cs.at[slot], self.cr.at[slot], device_id={"dp": self.by_core}, device_id_type=MESH)

    def copy_1(self, t, q):
        two, four = lax.rem(t, 2), lax.rem(t, 4)
        return pltpu.make_async_remote_copy(
            self.send_1.at[two, q], self.recv_1.at[four, q], self.s1.at[two, q], self.r1.at[four, q],
            device_id={"dp": self.by_y if q else self.by_x}, device_id_type=MESH)

    def copy_2(self, t, q):
        two, four = lax.rem(t, 2), lax.rem(t, 4)
        return pltpu.make_async_remote_copy(
            self.send_2.at[two, q], self.recv_2.at[four, q], self.s2.at[two, q], self.r2.at[four, q],
            device_id={"dp": self.by_x if q else self.by_y}, device_id_type=MESH)

    def middle(self, s):
        @pl.when((s >= 3) & (s <= NT + 2))
        def _():
            for q in range(2):
                self.copy_2(s - 3, q).start()

        @pl.when((s >= 1) & (s <= NT))
        def _():
            t = s - 1
            self.copy_c(t).wait()
            slot = lax.rem(t, 2)
            for q in range(2):
                mine = self.y if q else self.x
                for i in range(2):
                    away, here = 2 * (1 - mine) + i, 2 * mine + i
                    self.send_1[slot, q, i] = (self.keep_c[q, away] + self.recv_c[slot, q, away].astype(F32)).astype(BF)
                    self.keep_1[slot, q, i] = self.keep_c[q, here] + self.recv_c[slot, q, here].astype(F32)

    def end(self, s):
        @pl.when(s < NT)
        def _():
            self.copy_c(s).start()

        @pl.when((s >= 1) & (s <= NT))
        def _():
            for q in range(2):
                self.copy_1(s - 1, q).start()

        @pl.when(s >= 4)
        def _():
            t = s - 4
            two, four = lax.rem(t, 2), lax.rem(t, 4)
            squares = jnp.zeros((8, 128), F32)
            for q in range(2):
                self.copy_2(t, q).wait()
                g = (self.keep_2[two, q] + self.recv_2[four, q].astype(F32)).astype(BF)
                wide = g.astype(F32)
                squares += jnp.sum((wide * wide).reshape(48, 8, 128), 0)
                self.fin_ref[t, q, 0] = g[0]
                self.fin_ref[t, q, 1] = g[1]
                self.fin_ref[t, q, 2] = wide[2].T.astype(BF)
            self.ssq_ref[...] += squares

        @pl.when((s >= 2) & (s <= NT + 1))
        def _():
            t = s - 2
            two, four = lax.rem(t, 2), lax.rem(t, 4)
            for q in range(2):
                mine = self.x if q else self.y
                self.copy_1(t, q).wait()
                self.send_2[two, q] = (self.keep_1[two, q, 1 - mine] + self.recv_1[four, q, 1 - mine].astype(F32)).astype(BF)
                self.keep_2[two, q] = self.keep_1[two, q, mine] + self.recv_1[four, q, mine].astype(F32)

    def gradients(self, at_ref, dt_ref, dgate, dup, act):
        for half, to in ((1 - self.core, self.send_c), (self.core, self.keep_c)):
            rows = pl.ds(pl.multiple_of(half * 512, 512), 512)
            for i, (left, right) in enumerate(((at_ref, dgate), (at_ref, dup), (dt_ref, act))):
                out = dot(left[rows, :], right[...]).astype(to.dtype)
                for b in range(4):
                    for q in range(2):
                        to[q, b, i] = out[b * 128 : (b + 1) * 128, q * 128 : (q + 1) * 128]


def pieces(gate, up, dact):
    sig = lax.logistic(gate)
    silu = gate * sig
    dact = dact.astype(BF).astype(F32)
    act = (silu * up).astype(BF)
    dup = (dact * silu).astype(BF)
    dgate = (dact * up * (sig + silu * (1 - sig))).astype(BF)
    return act, dgate, dup


def backward_1_kernel(a_ref, dy_ref, at_ref, dyt_ref, h_ref, dyb_ref, wg_ref, wu_ref, wd_ref, fin_ref, ssq_ref, dh_ref, dht_ref, acc, act, dgate, dup, *comm):
    s = pl.program_id(0)
    scatter = Scatter(comm, fin_ref, ssq_ref)

    @pl.when(s == 0)
    def _():
        scatter.enter()
        acc[...] = jnp.zeros_like(acc)

    @pl.when(s < NT)
    def _():
        wg, wu, wd = wg_ref[0], wu_ref[0], wd_ref[0]
        for b in range(NB):
            rows = slice(b * BLOCK, (b + 1) * BLOCK)
            a = a_ref[rows, :]
            one, two, three = pieces(dot(a, wg), dot(a, wu), dot_t(dy_ref[rows, :], wd))
            act[rows, :], dgate[rows, :], dup[rows, :] = one, two, three
            acc[rows, :] += dot_t(two, wg) + dot_t(three, wu)

    scatter.middle(s)

    @pl.when(s < NT)
    def _():
        scatter.gradients(at_ref, dyt_ref, dgate, dup, act)

    @pl.when(s >= NT)
    def _():
        rows = pl.ds(pl.multiple_of((s - NT) * BLOCK, BLOCK), BLOCK)
        da = acc[rows, :].astype(BF).astype(F32)
        wide = h_ref[...].astype(F32)
        scale = scale_of(wide)
        inner = jnp.sum(da * wide, -1, keepdims=True)
        by_h = (da * scale - wide * (inner * (scale * scale * scale) * (1.0 / D))).astype(BF)
        dh = (dyb_ref[...].astype(F32) + by_h.astype(F32)).astype(BF)
        dh_ref[...] = dh
        dht_ref[...] = dh.T

    scatter.end(s)


def backward_0_kernel(dh_ref, at_ref, dht_ref, gate_ref, up_ref, wd_ref, fin_ref, ssq_ref, act, dgate, dup, *comm):
    s = pl.program_id(0)
    scatter = Scatter(comm, fin_ref, ssq_ref)

    @pl.when(s == 0)
    def _():
        scatter.enter()

    @pl.when(s < NT)
    def _():
        wd = wd_ref[0]
        for b in range(NB):
            rows = slice(b * BLOCK, (b + 1) * BLOCK)
            act[rows, :], dgate[rows, :], dup[rows, :] = pieces(gate_ref[rows, :], up_ref[rows, :], dot_t(dh_ref[rows, :], wd))

    scatter.middle(s)

    @pl.when(s < NT)
    def _():
        scatter.gradients(at_ref, dht_ref, dgate, dup, act)

    scatter.end(s)


FIN = jax.ShapeDtypeStruct((NT, 2, 3, 128, 128), BF)
SSQ = jax.ShapeDtypeStruct((8, 128), F32)


def backward(number, *operands):
    tile = lambda s: jnp.minimum(s, NT - 1)
    block = lambda s: jnp.clip(s - NT, 0, NB - 1)
    wspec = pl.BlockSpec((1, D, TILE), lambda s: (number, 0, tile(s)))
    dspec = pl.BlockSpec((1, TILE, D), lambda s: (number, tile(s), 0))
    fspec = pl.BlockSpec((T, TILE), lambda s: (0, tile(s)))
    rspec = pl.BlockSpec((BLOCK, D), lambda s: (block(s), 0))
    tspec = pl.BlockSpec((D, BLOCK), lambda s: (0, block(s)))
    out_shape, out_specs = [FIN, SSQ], [pl.BlockSpec(FIN.shape, lambda s: (0,) * 5), pl.BlockSpec((8, 128), lambda s: (0, 0))]
    scratch = [pltpu.VMEM((T, TILE), BF)] * 3
    if number == 1:
        kernel = backward_1_kernel
        in_specs = [whole((T, D)), whole((T, D)), whole((D, T)), whole((D, T)), rspec, rspec, wspec, wspec, dspec]
        out_shape += [jax.ShapeDtypeStruct((T, D), BF), jax.ShapeDtypeStruct((D, T), BF)]
        out_specs += [rspec, tspec]
        scratch = [pltpu.VMEM((T, D), F32)] + scratch
    else:
        kernel = backward_0_kernel
        in_specs = [whole((T, D)), whole((D, T)), whole((D, T)), fspec, fspec, dspec]
    return pl.pallas_call(
        kernel,
        grid=(NT + DRAIN,),
        in_specs=in_specs,
        out_specs=out_specs,
        out_shape=out_shape,
        scratch_shapes=scratch + COMM_SCRATCH,
        compiler_params=pltpu.CompilerParams(
            dimension_semantics=("arbitrary",), vmem_limit_bytes=VMEM_LIMIT, collective_id=number, has_side_effects=True),
        cost_estimate=pl.CostEstimate(flops=(16 if number else 8) * T * D * F, bytes_accessed=64 << 20, transcendentals=T * F),
        name=f"backward_{number}",
    )(*operands)


def owner(q, b):
    core, high, low = b // 4, (b // 2) % 2, b % 2
    x, y = (low, high) if q else (high, low)
    return 4 * x + 2 * y + core


def optimizer_kernel(n_alias, factor_ref, g_ref, *refs):
    ins, outs = refs[:9], refs[9 + n_alias :]
    factor = factor_ref[0, 0]
    for b in range(8):
        for q in range(2):
            for i in range(3):
                g = g_ref[owner(q, b), 0, q, i].astype(F32) * factor
                rows, columns = slice(b * 128, (b + 1) * 128), slice(q * 128, (q + 1) * 128)
                at = (0, columns, rows) if i == 2 else (0, rows, columns)
                w, m, v = (ins[3 * k + i][at] for k in range(3))
                m = 0.9 * m + 0.1 * g
                v = 0.95 * v + 0.05 * g * g
                w = w.astype(F32)
                w = (w - 0.02 * (m * lax.rsqrt(v + 1e-8) + 0.1 * w)).astype(BF)
                outs[i][at], outs[3 + i][at], outs[6 + i][at] = w, m, v


def optimizer(number, first, count, factor, g, arrays, so_far):
    wide = pl.BlockSpec((1, D, TILE), lambda s: (number, 0, first + s))
    tall = pl.BlockSpec((1, TILE, D), lambda s: (number, first + s, 0))
    three = [wide, wide, tall]
    so_far = list(so_far or ())
    out_shape = [jax.ShapeDtypeStruct(a.shape, a.dtype) for a in arrays]
    return pl.pallas_call(
        functools.partial(optimizer_kernel, len(so_far)),
        grid=(count,),
        in_specs=[pl.BlockSpec(memory_space=pltpu.SMEM), pl.BlockSpec((8, 1, 2, 3, 128, 128), lambda s: (0, s, 0, 0, 0, 0))]
        + three * 3 + [pl.BlockSpec(memory_space=pl.ANY)] * len(so_far),
        out_specs=three * 3,
        out_shape=out_shape,
        input_output_aliases={11 + i: i for i in range(len(so_far))},
        compiler_params=pltpu.CompilerParams(dimension_semantics=("arbitrary",), vmem_limit_bytes=VMEM_LIMIT),
        cost_estimate=pl.CostEstimate(flops=count * 20 * 3 * D * TILE, bytes_accessed=count * 22 * 3 * D * TILE, transcendentals=count * 3 * D * TILE),
        name=f"optimizer_{number}_{first}",
    )(factor, g, *arrays, *so_far)


def solution(mesh):
    def step(x, dy, *arrays):
        wg, wu, wd = arrays[:3]
        x, dy = x[0], dy[0]
        gate, up, h, a, a0t, at, dyt = forward(x, dy, wg, wu, wd)
        fin1, ssq1, dh, dht = backward(1, a, dy, at, dyt, h, dy, wg, wu, wd)
        fin0, ssq0 = backward(0, dh, a0t, dht, gate, up, wd)
        total = lax.psum(jnp.sum(ssq1 + ssq0), "dp")
        count = sum(w.size for w in arrays[:3])
        factor = jnp.minimum(1.0, 0.5 * lax.rsqrt(total / count + 1e-30)).reshape(1, 1)
        g1 = lax.all_gather(fin1, "dp")
        new = optimizer(1, 0, NT, factor, g1, arrays, None)
        cut = 5
        for first, count in ((0, cut), (cut, NT - cut)):
            g0 = lax.all_gather(fin0[first : first + count], "dp")
            new = optimizer(0, first, count, factor, g0, arrays, new)
        return tuple(new)

    return jax.shard_map(
        step,
        mesh=mesh,
        in_specs=(P(("rep", "dp"), None, None),) * 2 + (P(None, None, None),) * 9,
        out_specs=(P("rep", None, None),) * 9,
        check_vma=False,
    )
```

```python
import functools

import jax
import jax.numpy as jnp
from jax import lax
from jax.experimental import pallas as pl
from jax.experimental.pallas import tpu as pltpu
from jax.sharding import PartitionSpec as P


T, D, F, TILE = 2048, 1024, 2816, 256
NT = F // TILE
BLOCK = 512
CHUNK = 64
LANES = 128
PIECE = (3, LANES, LANES)
NB = T // BLOCK
DRAIN = 5
EARLY = 2
UNITS_1 = ((EARLY, 6), (6, NT))
UNITS_0 = ((0, 5), (5, NT))
STAGES = {10: "a0", 12: "a1", 15: "b0", 17: "b1", 20: "c0", 22: "c1 d0", 25: "d1"}
BF, F32 = jnp.bfloat16, jnp.float32
MESH = pl.DeviceIdType.MESH
VMEM_LIMIT = 62 * 1024 * 1024


def dot(a, b):
    return jnp.dot(a, b, preferred_element_type=F32)


def dot_t(a, b):
    return lax.dot_general(a, b, (((1,), (1,)), ((), ())), preferred_element_type=F32)


def whole(shape):
    zeros = (0,) * len(shape)
    return pl.BlockSpec(shape, lambda *_: zeros, pipeline_mode=pl.Buffered(1))


def scale_of(wide):
    return lax.rsqrt(jnp.mean(wide * wide, -1, keepdims=True) + 1e-6)


def forward_kernel(x_ref, dy_ref, wg_ref, wu_ref, wd_ref, gate_ref, up_ref, h_ref, a_ref, a0t_ref, at_ref, dyt_ref, a0, act, wd, sem):
    s = pl.program_id(0)
    load = pltpu.make_async_copy(wd_ref.at[0], wd, sem)

    @pl.when(s == 0)
    def _():
        load.start()
        for b in range(NB):
            rows = slice(b * BLOCK, (b + 1) * BLOCK)
            wide = x_ref[rows, :].astype(F32)
            a0[rows, :] = (wide * scale_of(wide)).astype(BF)

    @pl.when(s < NT)
    def _():
        columns = pl.ds(pl.multiple_of(s * TILE, TILE), TILE)
        wg, wu = wg_ref[0], wu_ref[0]
        for b in range(NB):
            rows = slice(b * BLOCK, (b + 1) * BLOCK)
            gate = dot(a0[rows, :], wg)
            up = dot(a0[rows, :], wu)
            gate_ref[0, rows, :] = gate
            up_ref[0, rows, :] = up
            act[rows, columns] = (gate * (0.5 * jnp.tanh(0.5 * gate) + 0.5) * up).astype(BF)

    @pl.when(s == NT)
    def _():
        load.wait()

    @pl.when(s >= NT)
    def _():
        rows = pl.ds(pl.multiple_of((s - NT) * BLOCK, BLOCK), BLOCK)
        out = dot(act[rows, :], wd[...]).astype(BF)
        h = (x_ref[rows, :].astype(F32) + out.astype(F32)).astype(BF)
        h_ref[...] = h
        wide = h.astype(F32)
        a = (wide * scale_of(wide)).astype(BF)
        a_ref[...] = a
        at_ref[...] = a.T
        a0t_ref[...] = a0[rows, :].T
        dyt_ref[...] = dy_ref[...].T


def forward(x, dy, wg, wu, wd):
    tile = lambda s: jnp.minimum(s, NT - 1)
    block = lambda s: jnp.maximum(s - NT, 0)
    wspec = pl.BlockSpec((1, D, TILE), lambda s: (0, 0, tile(s)))
    fspec = pl.BlockSpec((1, T, TILE), lambda s: (tile(s), 0, 0))
    rspec = pl.BlockSpec((BLOCK, D), lambda s: (block(s), 0))
    tspec = pl.BlockSpec((D, BLOCK), lambda s: (0, block(s)))
    flat = lambda shape, dtype: jax.ShapeDtypeStruct(shape, dtype)
    return pl.pallas_call(
        forward_kernel,
        grid=(NT + NB,),
        in_specs=[whole((T, D)), rspec, wspec, wspec, pl.BlockSpec(memory_space=pl.ANY)],
        out_specs=[fspec, fspec, rspec, rspec, tspec, tspec, tspec],
        out_shape=[
            flat((NT, T, TILE), F32), flat((NT, T, TILE), F32), flat((T, D), BF), flat((T, D), BF),
            flat((D, T), BF), flat((D, T), BF), flat((D, T), BF),
        ],
        scratch_shapes=[pltpu.VMEM((T, D), BF), pltpu.VMEM((T, F), BF), pltpu.VMEM((F, D), BF), pltpu.SemaphoreType.DMA],
        compiler_params=pltpu.CompilerParams(dimension_semantics=("arbitrary",), vmem_limit_bytes=VMEM_LIMIT),
        cost_estimate=pl.CostEstimate(flops=6 * T * D * F, bytes_accessed=100 << 20, transcendentals=T * F),
        name="forward",
    )(x, dy, wg, wu, wd)


COMM_SCRATCH = [
    pltpu.VMEM((2, 4, *PIECE), BF),
    pltpu.VMEM((2, 4, *PIECE), F32),
    pltpu.VMEM((2, 2, 4, *PIECE), BF),
    pltpu.VMEM((2, 2, 2, *PIECE), BF),
    pltpu.VMEM((2, 2, 2, *PIECE), F32),
    pltpu.VMEM((4, 2, 2, *PIECE), BF),
    pltpu.VMEM((2, 2, *PIECE), BF),
    pltpu.VMEM((2, 2, *PIECE), F32),
    pltpu.VMEM((4, 2, *PIECE), BF),
    pltpu.SemaphoreType.DMA((2,)),
    pltpu.SemaphoreType.DMA((2,)),
    pltpu.SemaphoreType.DMA((2, 2)),
    pltpu.SemaphoreType.DMA((4, 2)),
    pltpu.SemaphoreType.DMA((2, 2)),
    pltpu.SemaphoreType.DMA((4, 2)),
]


class Scatter:
    def __init__(self, refs, place, ssq_ref):
        (self.send_c, self.keep_c, self.recv_c, self.send_1, self.keep_1, self.recv_1, self.send_2, self.keep_2, self.recv_2,
         self.cs, self.cr, self.s1, self.r1, self.s2, self.r2) = refs
        self.place, self.ssq_ref = place, ssq_ref
        me = lax.axis_index("dp")
        self.core, self.y, self.x = lax.rem(me, 2), lax.rem(me // 2, 2), me // 4
        self.by_core, self.by_y, self.by_x = me + 1 - 2 * self.core, me + 2 - 4 * self.y, me + 4 - 8 * self.x

    def enter(self, others):
        barrier = pltpu.get_barrier_semaphore()
        for other in others:
            pl.semaphore_signal(barrier, inc=1, device_id={"dp": other}, device_id_type=MESH)
        pl.semaphore_wait(barrier, len(others))

    def copy_c(self, t):
        slot = lax.rem(t, 2)
        return pltpu.make_async_remote_copy(
            self.send_c, self.recv_c.at[slot], self.cs.at[slot], self.cr.at[slot], device_id={"dp": self.by_core}, device_id_type=MESH)

    def copy_1(self, t, q):
        two, four = lax.rem(t, 2), lax.rem(t, 4)
        return pltpu.make_async_remote_copy(
            self.send_1.at[two, q], self.recv_1.at[four, q], self.s1.at[two, q], self.r1.at[four, q],
            device_id={"dp": self.by_y if q else self.by_x}, device_id_type=MESH)

    def copy_2(self, t, q):
        two, four = lax.rem(t, 2), lax.rem(t, 4)
        return pltpu.make_async_remote_copy(
            self.send_2.at[two, q], self.recv_2.at[four, q], self.s2.at[two, q], self.r2.at[four, q],
            device_id={"dp": self.by_x if q else self.by_y}, device_id_type=MESH)

    def on(self, t):
        return pl.when((t >= 0) & (t < NT))

    def sums(self, first, second, third):
        @self.on(third)
        def _():
            t, two, four = third, lax.rem(third, 2), lax.rem(third, 4)
            squares = jnp.zeros((8, LANES), F32)
            for q in range(2):
                self.copy_2(t, q).wait()
                g = (self.keep_2[two, q] + self.recv_2[four, q].astype(F32)).astype(BF)
                wide = g.astype(F32)
                squares += jnp.sum((wide * wide).reshape(48, 8, LANES), 0)
                for start, stop, ref in self.place:

                    @pl.when((t >= start) & (t < stop))
                    def _():
                        ref[q, t - start, 0] = g[0]
                        ref[q, t - start, 1] = g[1]
                        ref[q, t - start, 2] = wide[2].T.astype(BF)

            self.ssq_ref[...] += squares

        @self.on(second)
        def _():
            two, four = lax.rem(second, 2), lax.rem(second, 4)
            for q in range(2):
                mine = self.x if q else self.y
                self.copy_1(second, q).wait()
                self.send_2[two, q] = (self.keep_1[two, q, 1 - mine] + self.recv_1[four, q, 1 - mine].astype(F32)).astype(BF)
                self.keep_2[two, q] = self.keep_1[two, q, mine] + self.recv_1[four, q, mine].astype(F32)

        @self.on(first)
        def _():
            self.copy_c(first).wait()
            slot = lax.rem(first, 2)
            for q in range(2):
                mine = self.y if q else self.x
                for i in range(2):
                    away, here = 2 * (1 - mine) + i, 2 * mine + i
                    self.send_1[slot, q, i] = (self.keep_c[q, away] + self.recv_c[slot, q, away].astype(F32)).astype(BF)
                    self.keep_1[slot, q, i] = self.keep_c[q, here] + self.recv_c[slot, q, here].astype(F32)

    def sends(self, first, second):
        @self.on(first)
        def _():
            for q in range(2):
                self.copy_1(first, q).start()

        @self.on(second)
        def _():
            for q in range(2):
                self.copy_2(second, q).start()

    def gradients(self, at_ref, dt_ref, dgate, dup, act, between=lambda: None):
        for half, to in ((1 - self.core, self.send_c), (self.core, self.keep_c)):
            rows = pl.ds(pl.multiple_of(half * 512, 512), 512)
            for i, (left, right) in enumerate(((at_ref, dgate), (at_ref, dup), (dt_ref, act))):
                out = dot(left[rows, :], right[...]).astype(to.dtype)
                for b in range(4):
                    for q in range(2):
                        to[q, b, i] = out[b * LANES : (b + 1) * LANES, q * LANES : (q + 1) * LANES]
            if to is self.send_c:
                between()


class Gather:
    def __init__(self, scatter, fin, g_ref, la, sa, ra, sb, rb, sc, rc):
        self.s, self.fin, self.g = scatter, fin, g_ref
        self.sems = la, sa, ra, sb, rb, sc, rc
        x, y, core = scatter.x, scatter.y, scatter.core
        self.mine = (4 * core + 2 * x + y, 4 * core + 2 * y + x)
        self.pair = (4 * core + 2 * x, 4 * core + 2 * y)

    def local(self, t, q):
        return pltpu.make_async_copy(self.fin.at[q, t], self.g.at[t, q, self.mine[q]], self.sems[0].at[t, q])

    def remote(self, t, q, source, target, sems, to):
        send, receive = sems
        return pltpu.make_async_remote_copy(source, target, send.at[t, q], receive.at[t, q], device_id={"dp": to}, device_id_type=MESH)

    def a(self, t, q):
        here = self.g.at[t, q, self.mine[q]]
        return self.remote(t, q, self.fin.at[q, t], here, self.sems[1:3], self.s.by_x if q else self.s.by_y)

    def b(self, t, q):
        here = self.g.at[t, q, pl.ds(self.pair[q], 2)]
        return self.remote(t, q, here, here, self.sems[3:5], self.s.by_y if q else self.s.by_x)

    def c(self, t, q):
        here = self.g.at[t, q, pl.ds(4 * self.s.core, 4)]
        return self.remote(t, q, here, here, self.sems[5:7], self.s.by_core)

    def step(self, s):
        for at, events in STAGES.items():

            @pl.when(s == at)
            def _():
                for stage, t in events.split():
                    t = int(t)
                    for q in range(2):
                        if stage == "a":
                            self.local(t, q).start()
                            self.a(t, q).start()
                        elif stage == "b":
                            self.local(t, q).wait()
                            self.a(t, q).wait()
                            self.b(t, q).start()
                        elif stage == "c":
                            self.b(t, q).wait()
                            self.c(t, q).start()
                        else:
                            self.c(t, q).wait()


def pieces(gate, up, dact):
    sig = 0.5 * jnp.tanh(0.5 * gate) + 0.5
    silu = gate * sig
    dact = dact.astype(BF).astype(F32)
    act = (silu * up).astype(BF)
    dup = (dact * silu).astype(BF)
    dgate = (dact * up * (sig + silu * (1 - sig))).astype(BF)
    return act, dgate, dup


def backward_1_kernel(
    a_hbm, dy_hbm, at_hbm, dyt_hbm, h_ref, dyb_ref, wg_ref, wu_ref, wd_ref,
    *refs,
):
    fins, refs = refs[: len(UNITS_1)], refs[len(UNITS_1) :]
    (g_ref, ssq_ref, dh_ref, dht_ref, kept,
     a_ref, dy_ref, at_ref, dyt_ref, loads, acc, act, dgate, dup, again, saves, reads, fin, la, sa, ra, sb, rb, sc, rc, *comm) = refs
    s = pl.program_id(0)
    scatter = Scatter(comm, [(0, EARLY, fin)] + [(*unit, ref) for unit, ref in zip(UNITS_1, fins, strict=True)], ssq_ref)
    gather = Gather(scatter, fin, g_ref, la, sa, ra, sb, rb, sc, rc)
    load = [
        pltpu.make_async_copy(source, target, loads.at[i])
        for i, (source, target) in enumerate(((a_hbm, a_ref), (dy_hbm, dy_ref), (at_hbm, at_ref), (dyt_hbm, dyt_ref)))
    ]

    def save(t, i, source):
        return pltpu.make_async_copy(source, kept.at[t, i], saves.at[i])

    def read(t):
        slot = lax.rem(t, 2)
        return pltpu.make_async_copy(kept.at[t], again.at[slot], reads.at[slot])

    @pl.when(s == 0)
    def _():
        for one in load:
            one.start()
        acc[...] = jnp.zeros_like(acc)
        ssq_ref[...] = jnp.zeros_like(ssq_ref)
        scatter.enter((scatter.by_core, scatter.by_y, scatter.by_x))
        load[0].wait()
        load[1].wait()

    @pl.when(s < NT)
    def _():
        wg, wu, wd = wg_ref[0], wu_ref[0], wd_ref[0]
        for b in range(NB):
            rows = slice(b * BLOCK, (b + 1) * BLOCK)
            a = a_ref[rows, :]
            one, two, three = pieces(dot(a, wg), dot(a, wu), dot_t(dy_ref[rows, :], wd))
            act[rows, :], dgate[rows, :], dup[rows, :] = one, two, three

    @pl.when(s == 0)
    def _():
        load[2].wait()
        load[3].wait()

    @pl.when(s < NT)
    def _():
        scatter.sums(s - 1, s - 3, s - 5)
        for i, source in enumerate((dgate, dup)):
            save(s, i, source).start()
        scatter.gradients(at_ref, dyt_ref, dgate, dup, act)
        for i, source in enumerate((dgate, dup)):
            save(s, i, source).wait()
        scatter.copy_c(s).start()
        scatter.sends(s - 1, s - 3)

    @pl.when((s >= NT - 1) & (s < 2 * NT - 1))
    def _():
        read(s - (NT - 1)).start()

    @pl.when((s >= NT) & (s < 2 * NT))
    def _():
        tile = s - NT
        read(tile).wait()
        slot = lax.rem(tile, 2)
        both = jnp.concatenate([wg_ref[0], wu_ref[0]], 1)
        for b in range(NB):
            rows = slice(b * BLOCK, (b + 1) * BLOCK)
            acc[rows, :] += dot_t(jnp.concatenate([again[slot, 0, rows, :], again[slot, 1, rows, :]], 1), both)

        @pl.when((lax.rem(tile, 2) == 1) & (tile < 2 * DRAIN))
        def _():
            later = NT + tile // 2
            scatter.sums(later - 1, later - 3, later - 5)
            scatter.sends(later - 1, later - 3)

    @pl.when(s >= 2 * NT)
    def _():
        rows = pl.ds(pl.multiple_of((s - 2 * NT) * BLOCK, BLOCK), BLOCK)
        da = acc[rows, :].astype(BF).astype(F32)
        wide = h_ref[...].astype(F32)
        scale = scale_of(wide)
        inner = jnp.sum(da * wide, -1, keepdims=True)
        by_h = (da * scale - wide * (inner * (scale * scale * scale) * (1.0 / D))).astype(BF)
        dh = (dyb_ref[...].astype(F32) + by_h.astype(F32)).astype(BF)
        dh_ref[...] = dh
        dht_ref[...] = dh.T

    gather.step(s)


def backward_0_kernel(count, dh_hbm, at_hbm, dht_hbm, gate_ref, up_ref, wd_ref, ssq_1_ref, *refs):
    s = pl.program_id(0)
    fins, refs = refs[: len(UNITS_0)], refs[len(UNITS_0) :]
    factor_ref, dh_ref, at_ref, dht_ref, loads, act, dgate, dup, ssq, send, recv, squares, *comm = refs
    scatter = Scatter(comm, [(*unit, ref) for unit, ref in zip(UNITS_0, fins, strict=True)], ssq)
    load = [
        pltpu.make_async_copy(source, target, loads.at[i])
        for i, (source, target) in enumerate(((dh_hbm, dh_ref), (at_hbm, at_ref), (dht_hbm, dht_ref)))
    ]
    me = lax.axis_index("dp")
    others = [lax.rem(me + i, 8) for i in range(1, 8)]

    def tell(i):
        return pltpu.make_async_remote_copy(
            ssq, squares.at[me], send.at[i], recv.at[me], device_id={"dp": others[i]}, device_id_type=MESH)

    def hear(i):
        return pltpu.make_async_remote_copy(
            ssq, squares.at[others[i]], send.at[i], recv.at[others[i]], device_id={"dp": others[i]}, device_id_type=MESH)

    @pl.when(s == 0)
    def _():
        for one in load:
            one.start()
        ssq[...] = ssq_1_ref[...]
        scatter.enter(others)
        load[0].wait()

    @pl.when(s < NT)
    def _():
        wd = wd_ref[0]
        for b in range(NB):
            rows = slice(b * BLOCK, (b + 1) * BLOCK)
            act[rows, :], dgate[rows, :], dup[rows, :] = pieces(gate_ref[0, rows, :], up_ref[0, rows, :], dot_t(dh_ref[rows, :], wd))

    @pl.when(s == 0)
    def _():
        load[1].wait()
        load[2].wait()

    scatter.sums(s - 1, s - 3, s - 5)

    @pl.when(s < NT)
    def _():
        scatter.gradients(at_ref, dht_ref, dgate, dup, act)
        scatter.copy_c(s).start()

    scatter.sends(s - 1, s - 3)

    @pl.when(s == NT + DRAIN - 1)
    def _():
        for i in range(7):
            tell(i).start()
        squares[me] = ssq[...]
        for i in range(7):
            tell(i).wait_send()
            hear(i).wait_recv()
        total = squares[0]
        for i in range(1, 8):
            total += squares[i]
        total = jnp.broadcast_to(jnp.sum(total, keepdims=True), (8, LANES))
        factor_ref[...] = jnp.minimum(1.0, 0.5 * lax.rsqrt(total / count + 1e-30))


def backward(number, *operands):
    steps = 2 * NT + NB if number else NT + DRAIN
    tile = lambda s: jnp.minimum(s, NT - 1)
    twice = lambda s: jnp.where(s < NT, s, jnp.minimum(s - NT, NT - 1))
    block = lambda s: jnp.clip(s - 2 * NT, 0, NB - 1)
    anywhere = pl.BlockSpec(memory_space=pl.ANY)
    wspec = pl.BlockSpec((1, D, TILE), lambda s: (number, 0, twice(s)))
    dspec = pl.BlockSpec((1, TILE, D), lambda s: (number, tile(s), 0))
    fspec = pl.BlockSpec((1, T, TILE), lambda s: (tile(s), 0, 0))
    rspec = pl.BlockSpec((BLOCK, D), lambda s: (block(s), 0))
    tspec = pl.BlockSpec((D, BLOCK), lambda s: (0, block(s)))
    small = pl.BlockSpec((8, LANES), lambda s: (0, 0))
    shape = jax.ShapeDtypeStruct
    fin = [shape((2, last - first, *PIECE), BF) for first, last in (UNITS_1 if number else UNITS_0)]
    fins = [pl.BlockSpec(one.shape, lambda s: (0, 0, 0, 0, 0)) for one in fin]
    dma = pltpu.SemaphoreType.DMA
    scratch = [pltpu.VMEM((T, TILE), BF)] * 3
    if number == 1:
        kernel = backward_1_kernel
        in_specs = [anywhere] * 4 + [rspec, rspec, wspec, wspec, dspec]
        out_shape = fin + [
            shape((EARLY, 2, 8, *PIECE), BF), shape((8, LANES), F32), shape((T, D), BF), shape((D, T), BF), shape((NT, 2, T, TILE), BF)]
        out_specs = fins + [anywhere, small, rspec, tspec, anywhere]
        scratch = (
            [pltpu.VMEM((T, D), BF)] * 2 + [pltpu.VMEM((D, T), BF)] * 2 + [dma((4,)), pltpu.VMEM((T, D), F32)] + scratch
            + [pltpu.VMEM((2, 2, T, TILE), BF), dma((2,)), dma((2,))] + [pltpu.VMEM((2, EARLY, *PIECE), BF)] + [dma((EARLY, 2))] * 7 + COMM_SCRATCH
        )
    else:
        kernel = functools.partial(backward_0_kernel, float(2 * 3 * D * F))
        in_specs = [anywhere] * 3 + [fspec, fspec, dspec, small]
        out_shape, out_specs = fin + [shape((8, LANES), F32)], fins + [small]
        scratch = (
            [pltpu.VMEM((T, D), BF)] + [pltpu.VMEM((D, T), BF)] * 2 + [dma((3,))] + scratch
            + [pltpu.VMEM((8, LANES), F32), dma((7,)), dma((8,)), pltpu.VMEM((8, 8, LANES), F32)] + COMM_SCRATCH
        )
    return pl.pallas_call(
        kernel,
        grid=(steps,),
        in_specs=in_specs,
        out_specs=out_specs,
        out_shape=out_shape,
        scratch_shapes=scratch,
        compiler_params=pltpu.CompilerParams(
            dimension_semantics=("arbitrary",), vmem_limit_bytes=VMEM_LIMIT, collective_id=number, has_side_effects=True),
        cost_estimate=pl.CostEstimate(flops=(16 if number else 8) * T * D * F, bytes_accessed=64 << 20, transcendentals=T * F),
    )(*operands)


def optimizer_kernel(n_g, n_alias, factor_ref, *refs):
    gs, ins, outs = refs[:n_g], refs[n_g : n_g + 9], refs[n_g + 9 + n_alias :]
    factor = factor_ref[0:1, :]

    def update(g_ref, at_g, rows, columns):
        for i in range(3):
            g = g_ref[i, at_g].astype(F32) * factor
            at = (0, *(columns if i == 2 else rows))
            w, m, v = (ins[3 * k + i][at] for k in range(3))
            m = 0.9 * m + 0.1 * g
            v = 0.95 * v + 0.05 * g * g
            w = w.astype(F32)
            w = (w - 0.02 * (m * lax.rsqrt(v + 1e-8) + 0.1 * w)).astype(BF)
            outs[i][at], outs[3 + i][at], outs[6 + i][at] = w, m, v

    if n_g == 1:
        parts = [(gs[0].at[0, q, b], q, LANES * b) for b in range(8) for q in range(2)]
    else:
        me = lax.axis_index("dp")
        core, y, x = lax.rem(me, 2), lax.rem(me // 2, 2), me // 4
        parts = []
        for side in range(2):
            at_core = 1 - core if side else core
            for i, (far_y, far_x) in enumerate(SIDES):
                at_y, at_x = 1 - y if far_y else y, 1 - x if far_x else x
                for q in range(2):
                    g_ref = gs[5 * side + 3 + q].at[0] if i == 3 else gs[5 * side + i].at[q, 0]
                    parts.append((g_ref, q, pl.multiple_of(LANES * (4 * at_core + (2 * at_y + at_x if q else 2 * at_x + at_y)), LANES)))
    for g_ref, q, b in parts:

        @pl.loop(0, LANES // CHUNK)
        def _(c):
            at_g = pl.ds(pl.multiple_of(c * CHUNK, CHUNK), CHUNK)
            rows = pl.ds(pl.multiple_of(b + c * CHUNK, CHUNK), CHUNK), slice(q * LANES, (q + 1) * LANES)
            columns = pl.ds(pl.multiple_of(q * LANES + c * CHUNK, CHUNK), CHUNK), pl.ds(b, LANES)
            update(g_ref, at_g, rows, columns)


def optimizer(number, first, start, count, factor, gs, arrays, so_far):
    wide = pl.BlockSpec((1, D, TILE), lambda s: (number, 0, first + s))
    tall = pl.BlockSpec((1, TILE, D), lambda s: (number, first + s, 0))
    three = [wide, wide, tall]
    so_far = list(so_far or ())
    if len(gs) == 1:
        gspecs = [pl.BlockSpec((1, 2, 8, *PIECE), lambda s: (start + s, 0, 0, 0, 0, 0))]
    else:
        stacked = pl.BlockSpec((2, 1, *PIECE), lambda s: (0, start + s, 0, 0, 0))
        gspecs = ([stacked] * 3 + [pl.BlockSpec((1, *PIECE), lambda s: (start + s, 0, 0, 0))] * 2) * 2
    out_shape = [jax.ShapeDtypeStruct(a.shape, a.dtype) for a in arrays]
    return pl.pallas_call(
        functools.partial(optimizer_kernel, len(gs), len(so_far)),
        grid=(count,),
        in_specs=[pl.BlockSpec((8, LANES), lambda s: (0, 0))] + gspecs + three * 3 + [pl.BlockSpec(memory_space=pl.ANY)] * len(so_far),
        out_specs=three * 3,
        out_shape=out_shape,
        input_output_aliases={10 + len(gs) + i: i for i in range(len(so_far))},
        compiler_params=pltpu.CompilerParams(dimension_semantics=("arbitrary",), vmem_limit_bytes=VMEM_LIMIT),
        cost_estimate=pl.CostEstimate(flops=count * 6 * 10**8, bytes_accessed=count * 22 * 3 * D * TILE, transcendentals=count * 3 * D * TILE),
    )(factor, *gs, *arrays, *so_far)


SIDES = ((0, 0), (1, 0), (0, 1), (1, 1))

ONE, TWO, FAR = range(3)
PLAN = (
    (1, 0, 2, -1, [(TWO, 0), (ONE, 1)]),
    (1, 2, 4, 0, [(FAR, 0)]),
    (1, 4, 6, 0, [(TWO, 1), (ONE, 2)]),
    (1, 6, 9, 1, [(FAR, 1)]),
    (1, 9, 11, 1, [(TWO, 2), (ONE, 3)]),
    (0, 0, 3, 2, [(FAR, 2)]),
    (0, 3, 5, 2, [(TWO, 3)]),
    (0, 5, 11, 3, [(FAR, 3)]),
)


def swap(v, bit):
    return lax.ppermute(v, "dp", [(i, i ^ bit) for i in range(8)])


def solution(mesh):
    def step(x, dy, *arrays):
        wg, wu, wd = arrays[:3]
        x, dy = x[0], dy[0]
        gate, up, h, a, a0t, at, dyt = forward(x, dy, wg, wu, wd)
        *late, g1, ssq1, dh, dht, _ = backward(1, a, dy, at, dyt, h, dy, wg, wu, wd)
        one_hop = lambda v: [swap(v, 2), swap(v, 4)]
        other_core = lambda values: [swap(v, 1) for v in values]
        ahead = one_hop(late[0])
        *fin, factor = backward(0, dh, a0t, dht, gate, up, wd, ssq1)
        tie = lax.optimization_barrier
        late, ahead, factor = tie((late, ahead, factor))
        units = [(1, *unit) for unit in UNITS_1] + [(0, *unit) for unit in UNITS_0]
        own, one, two, far = late + fin, {0: ahead}, {}, {}

        far[0] = other_core([own[0]])
        new = None
        for number, first, last, u, opens in PLAN:
            if new:
                values = tie((new, [(own, one, two)[stage][i] for stage, i in opens]))
                new = values[0]
                for (stage, i), value in zip(opens, values[1], strict=True):
                    (own, one, two)[stage][i] = value
            for stage, i in opens:
                if stage == ONE:
                    one[i] = one_hop(own[i])
                    far[i] = other_core([own[i]])
                elif stage == TWO:
                    p, q = one[i][0][0], one[i][1][1]
                    two[i] = [swap(p, 4), swap(q, 2)]
                    far[i] = far[i] + other_core(one[i])
                else:
                    far[i] = far[i] + other_core(two[i])
            if u < 0:
                start, gs = first, [g1]
            else:
                start, gs = first - units[u][1], [own[u], *one[u], *two[u], *far[u]]
            new = optimizer(number, first, start, last - first, factor, gs, arrays, new)
        return tuple(new)

    return jax.shard_map(
        step,
        mesh=mesh,
        in_specs=(P(("rep", "dp"), None, None),) * 2 + (P(None, None, None),) * 9,
        out_specs=(P("rep", None, None),) * 9,
        check_vma=False,
    )
```
